16 devices in a mesh: dz: 2 (over z), dy: 2 (over y), dx: 4 (over x, core).
Axes of the slice: x: 2, y: 2, z: 2, core: 2. Of those that a mesh axis runs over, the one named last changes fastest.
Arguments:
- x_one: bfloat16 [32768, 1024], P(('dz', 'dy', 'dx'))
- g_one: bfloat16 [32768, 1024], P(('dz', 'dy', 'dx'))
- x_two: bfloat16 [32768, 1024], P(('dz', 'dy', 'dx'))
- g_two: bfloat16 [32768, 1024], P(('dz', 'dy', 'dx'))
- w_one: bfloat16 [1024, 2816], replicated
- w_two: bfloat16 [2816, 1024], replicated
- w_three: bfloat16 [1024, 2816], replicated
- w_four: bfloat16 [2816, 1024], replicated
Outputs:
- output 1: float32 [1024, 2816], replicated
- output 2: float32 [2816, 1024], replicated
- output 3: float32 [1024, 2816], replicated
- output 4: float32 [2816, 1024], replicated
- output 5: bfloat16 [32768, 1024], P(('dz', 'dy', 'dx'))
- output 6: bfloat16 [32768, 1024], P(('dz', 'dy', 'dx'))
All inputs are finite; a program needn't handle non-finite values.
Results may differ from the reference program's by a relative error of at most 0.00348054.
Values are sent between devices in bfloat16 or wider.
A program may use at most 1 GiB of HBM per device.

```python
import jax
import jax.numpy as jnp
from jax import lax

D = 1024
FF = 2816
TOKENS_DEV = 2048
DEVICES = 16

GELU_C = 0.7978845608028654
GELU_A = 0.044715


def gelu_value(pre_act):
    pre_f = pre_act.astype(jnp.float32)
    return 0.5 * pre_f * (1.0 + jnp.tanh(GELU_C * (pre_f + GELU_A * pre_f * pre_f * pre_f)))


def gelu_slope(pre_act):
    pre_f = pre_act.astype(jnp.float32)
    tanh_val = jnp.tanh(GELU_C * (pre_f + GELU_A * pre_f * pre_f * pre_f))
    return 0.5 * (1.0 + tanh_val) + 0.5 * pre_f * (1.0 - tanh_val * tanh_val) * GELU_C * (1.0 + 3.0 * GELU_A * pre_f * pre_f)


def local_grads(x_rows, g_rows, w_one, w_two, w_three, w_four):
    pre_one = jnp.dot(x_rows, w_one, preferred_element_type=jnp.float32).astype(jnp.bfloat16)
    act_one = gelu_value(pre_one).astype(jnp.bfloat16)
    act_two = (jnp.dot(act_one, w_two, preferred_element_type=jnp.float32) + x_rows.astype(jnp.float32)).astype(jnp.bfloat16)
    pre_three = jnp.dot(act_two, w_three, preferred_element_type=jnp.float32).astype(jnp.bfloat16)
    act_three = gelu_value(pre_three).astype(jnp.bfloat16)
    grad_four = jnp.dot(act_three.T, g_rows, preferred_element_type=jnp.float32)
    dz_three = (jnp.dot(g_rows, w_four.T, preferred_element_type=jnp.float32) * gelu_slope(pre_three)).astype(jnp.bfloat16)
    grad_three = jnp.dot(act_two.T, dz_three, preferred_element_type=jnp.float32)
    dh_two = (jnp.dot(dz_three, w_three.T, preferred_element_type=jnp.float32) + g_rows.astype(jnp.float32)).astype(jnp.bfloat16)
    grad_two = jnp.dot(act_one.T, dh_two, preferred_element_type=jnp.float32)
    dz_one = (jnp.dot(dh_two, w_two.T, preferred_element_type=jnp.float32) * gelu_slope(pre_one)).astype(jnp.bfloat16)
    grad_one = jnp.dot(x_rows.T, dz_one, preferred_element_type=jnp.float32)
    dx_rows = (jnp.dot(dz_one, w_one.T, preferred_element_type=jnp.float32) + dh_two.astype(jnp.float32)).astype(jnp.bfloat16)
    return (grad_one, grad_two, grad_three, grad_four), dx_rows


def setup_inputs(seed: int = 0) -> dict:
    sub_keys = jax.random.split(jax.random.key(seed), 8)
    total_rows = DEVICES * TOKENS_DEV

    def normal_bf16(sub_key, shape, scale):
        return (jax.random.normal(sub_key, shape, jnp.float32) * scale).astype(jnp.bfloat16)

    return {
        "x_one": normal_bf16(sub_keys[0], (total_rows, D), 1.0),
        "g_one": normal_bf16(sub_keys[1], (total_rows, D), 1.0),
        "x_two": normal_bf16(sub_keys[2], (total_rows, D), 1.0),
        "g_two": normal_bf16(sub_keys[3], (total_rows, D), 1.0),
        "w_one": normal_bf16(sub_keys[4], (D, FF), D ** -0.5),
        "w_two": normal_bf16(sub_keys[5], (FF, D), FF ** -0.5),
        "w_three": normal_bf16(sub_keys[6], (D, FF), D ** -0.5),
        "w_four": normal_bf16(sub_keys[7], (FF, D), FF ** -0.5),
    }


def reference(x_one, g_one, x_two, g_two, w_one, w_two, w_three, w_four):
    block_shape = (DEVICES, TOKENS_DEV, D)
    blocks_in = (x_one.reshape(block_shape), g_one.reshape(block_shape), x_two.reshape(block_shape), g_two.reshape(block_shape))

    def device_step(acc_grads, block_in):
        x_first, g_first, x_second, g_second = block_in
        grads_first, dx_first = local_grads(x_first, g_first, w_one, w_two, w_three, w_four)
        grads_second, dx_second = local_grads(x_second, g_second, w_one, w_two, w_three, w_four)
        new_acc = tuple(acc_part + grad_a + grad_b for acc_part, grad_a, grad_b in zip(acc_grads, grads_first, grads_second))
        return new_acc, (dx_first, dx_second)

    zero_grads = (jnp.zeros((D, FF), jnp.float32), jnp.zeros((FF, D), jnp.float32), jnp.zeros((D, FF), jnp.float32), jnp.zeros((FF, D), jnp.float32))
    sum_grads, dx_blocks = lax.scan(device_step, zero_grads, blocks_in)
    mean_grads = [total_grad / DEVICES for total_grad in sum_grads]
    dx_first_all = dx_blocks[0].reshape(DEVICES * TOKENS_DEV, D)
    dx_second_all = dx_blocks[1].reshape(DEVICES * TOKENS_DEV, D)
    return (mean_grads[0], mean_grads[1], mean_grads[2], mean_grads[3], dx_first_all, dx_second_all)
```

```python
import jax
import jax.numpy as jnp
from jax import lax
from jax.experimental import pallas as pl
from jax.experimental.pallas import tpu as pltpu
from jax.sharding import PartitionSpec as P

GELU_C = 0.7978845608028654
GELU_A = 0.044715
AXES = ("dz", "dy", "dx")
BF16 = jnp.bfloat16
F32 = jnp.float32
VMEM_LIMIT = 64000000
MESH = pl.DeviceIdType.MESH
CHUNK = 256
SLOTS = 5
CUTS_UPPER = (0, 11)
CUTS_LOWER = (0, 6, 11)
COLOUR_AXES = ((2, 1, 0), (1, 0, 2), (0, 2, 1))


def gelu_value(pre_act):
    pre_f = pre_act.astype(F32)
    return 0.5 * pre_f * (1.0 + jnp.tanh(GELU_C * (pre_f + GELU_A * pre_f * pre_f * pre_f)))


def dot_nn(lhs, rhs):
    return lax.dot_general(lhs, rhs, (((1,), (0,)), ((), ())), preferred_element_type=F32)


def dot_nt(lhs, rhs):
    return lax.dot_general(lhs, rhs, (((1,), (1,)), ((), ())), preferred_element_type=F32)


def dot_tn(lhs, rhs):
    return lax.dot_general(lhs, rhs, (((0,), (0,)), ((), ())), preferred_element_type=F32)


class Reducer:
    def __init__(self, rows, cols, by_rows, small):
        self.rows, self.cols, self.by_rows = rows, cols, by_rows
        tiles, unit = (rows // 8, 8) if by_rows else (cols // 128, 128)
        base, extra = tiles // 3, tiles % 3
        order = [(small + 1 + k) % 3 for k in range(3)]
        sizes = [0, 0, 0]
        for pos, colour in enumerate(order):
            sizes[colour] = (base + (1 if pos < extra else 0)) * unit
        self.parts = [(sum(sizes[:k]), sizes[k]) for k in range(3)]

    def scratch(self):
        bufs = [
            pltpu.VMEM((SLOTS, 2, 2, 2, 2, self.rows, self.cols), F32),
            pltpu.VMEM((2, 2, 2, 2, self.rows, self.cols), F32),
        ]
        for _, size in self.parts:
            block = (size, self.cols) if self.by_rows else (self.rows, size)
            bufs += [pltpu.VMEM((2,) + (2,) * (2 - level) + block, F32) for level in range(3)]
        return bufs + [pltpu.SemaphoreType.DMA((2, 10)), pltpu.SemaphoreType.DMA((2, 10))]

    N_SCRATCH = 13

    def bind(self, refs, place):
        self.part, self.recv0 = refs[0], refs[1]
        self.land = [refs[2 + 3 * k : 5 + 3 * k] for k in range(3)]
        self.send_sem, self.recv_sem = refs[11], refs[12]
        self.core, self.coord, self.partner, self.neighbour = place

    def put(self, chunk, value):
        self.part[lax.rem(chunk, SLOTS)] = value.reshape(2, 2, 2, 2, self.rows, self.cols)

    def core_copy(self, chunk):
        par = lax.rem(chunk, 2)
        return pltpu.make_async_remote_copy(
            self.part.at[lax.rem(chunk, SLOTS), :, :, :, 1 - self.core], self.recv0.at[par],
            self.send_sem.at[par, 9], self.recv_sem.at[par, 9], device_id=self.partner, device_id_type=MESH,
        )

    def where(self, chunk, colour, level, other):
        order = COLOUR_AXES[colour]
        index = [slice(None)] * 3
        for pos in range(level + 1):
            axis = order[pos]
            index[axis] = 1 - self.coord[axis] if (other and pos == level) else self.coord[axis]
        start, size = self.parts[colour]
        tail = (pl.ds(start, size), slice(None)) if self.by_rows else (slice(None), pl.ds(start, size))
        return (lax.rem(chunk, SLOTS),) + tuple(index) + (self.core,) + tail

    def chip_copy(self, chunk, colour, level):
        slot, par = 3 * colour + level, lax.rem(chunk, 2)
        return pltpu.make_async_remote_copy(
            self.part.at[self.where(chunk, colour, level, True)], self.land[colour][level].at[par],
            self.send_sem.at[par, slot], self.recv_sem.at[par, slot],
            device_id=self.neighbour[COLOUR_AXES[colour][level]], device_id_type=MESH,
        )

    def send(self, chunk, stage):
        if stage == 0:
            self.core_copy(chunk).start()
        else:
            for colour in range(3):
                self.chip_copy(chunk, colour, stage - 1).start()

    def add(self, chunk, stage):
        slot, par = lax.rem(chunk, SLOTS), lax.rem(chunk, 2)
        if stage == 0:
            self.core_copy(chunk).wait()
            for z in range(2):
                for y in range(2):
                    self.part[slot, z, y, :, self.core] = self.part[slot, z, y, :, self.core] + self.recv0[par, z, y]
        else:
            for colour in range(3):
                self.chip_copy(chunk, colour, stage - 1).wait()
                mine = self.where(chunk, colour, stage - 1, False)
                self.part[mine] = self.part[mine] + self.land[colour][stage - 1][par]

    def result(self, chunk):
        return self.part[(lax.rem(chunk, SLOTS),) + tuple(self.coord) + (self.core,)] * (1.0 / 16.0)


def whole(shape):
    return pl.BlockSpec(shape, lambda i: (0,) * len(shape), pipeline_mode=pl.Buffered(1))


def row_block(tile, cols):
    return pl.BlockSpec((tile, cols), lambda i: (i, 0))


def shape_of(shape, dtype):
    return jax.ShapeDtypeStruct(shape, dtype)


def cost(flops):
    return pl.CostEstimate(flops=flops, bytes_accessed=60000000, transcendentals=0)


def forward(x_one, x_two, g_one, g_two, w_one, w_two):
    half, d = x_one.shape
    f = w_one.shape[1]
    rows, tile = 2 * half, 256
    switch = half // tile

    def kernel(x1, x2, g1, g2, w1, w2, xc, gc, p1, h2, act):
        step = pl.program_id(0)

        @pl.when(step < switch)
        def _():
            xc[...] = x1[...]
            gc[...] = g1[...]

        @pl.when(step >= switch)
        def _():
            xc[...] = x2[...]
            gc[...] = g2[...]

        for j in range(f // CHUNK):
            cs = pl.ds(j * CHUNK, CHUNK)
            pre = dot_nn(xc[...], w1[:, cs]).astype(BF16)
            p1[:, cs] = pre
            act[:, cs] = gelu_value(pre).astype(BF16)
        h2[...] = (dot_nn(act[...], w2[...]) + xc[...].astype(F32)).astype(BF16)

    first = pl.BlockSpec((tile, d), lambda i: (jnp.minimum(i, switch - 1), 0))
    second = pl.BlockSpec((tile, d), lambda i: (jnp.maximum(i - switch, 0), 0))
    narrow = shape_of((rows, d), BF16)
    return pl.pallas_call(
        kernel,
        name="forward",
        grid=(rows // tile,),
        in_specs=[first, second, first, second, whole((d, f)), whole((f, d))],
        out_specs=[row_block(tile, d), row_block(tile, d), row_block(tile, f), row_block(tile, d)],
        out_shape=[narrow, narrow, shape_of((rows, f), BF16), narrow],
        scratch_shapes=[pltpu.VMEM((tile, f), BF16)],
        cost_estimate=cost(4 * rows * d * f),
        compiler_params=pltpu.CompilerParams(vmem_limit_bytes=VMEM_LIMIT),
    )(x_one, x_two, g_one, g_two, w_one, w_two)


def column_grads(act, grad, w_up, pre, w_down, low, count, ident):
    rows, d = act.shape
    tall = Reducer(CHUNK // 16, d, False, 2)
    wide = Reducer(d // 16, CHUNK, True, 0)
    tile = 512

    def kernel(act_ref, grad_ref, src_ref, down_ref, dz_ref, tall_ref, wide_ref, hid, *refs):
        step = pl.program_id(0)
        dx_pos = lax.axis_index("dx")
        core = lax.rem(dx_pos, 2)
        coord = [lax.axis_index("dz"), lax.axis_index("dy"), dx_pos // 2]
        partner = {"dx": dx_pos + 1 - 2 * core}
        neighbour = [{"dz": 1 - coord[0]}, {"dy": 1 - coord[1]}, {"dx": lax.rem(dx_pos + 2, 4)}]
        place = (core, coord, partner, neighbour)
        tall.bind(refs[: Reducer.N_SCRATCH], place)
        wide.bind(refs[Reducer.N_SCRATCH :], place)
        barrier = pltpu.get_barrier_semaphore()

        @pl.when(step == 0)
        def _():
            for other in [partner] + neighbour:
                pl.semaphore_signal(barrier, inc=1, device_id=other, device_id_type=MESH)

        @pl.when(step < count)
        def _():
            for r in range(rows // tile):
                rs = pl.ds(r * tile, tile)
                if pre is None:
                    val = dot_nn(act_ref[rs, :], src_ref[...]).astype(BF16).astype(F32)
                else:
                    val = src_ref[rs, :].astype(F32)
                tanh_val = jnp.tanh(GELU_C * (val + GELU_A * val * val * val))
                hid[rs, :] = (0.5 * val * (1.0 + tanh_val)).astype(BF16)
                slope = 0.5 * (1.0 + tanh_val) + 0.5 * val * (1.0 - tanh_val * tanh_val) * GELU_C * (1.0 + 3.0 * GELU_A * val * val)
                dz_ref[rs, :] = (dot_nt(grad_ref[rs, :], down_ref[...]) * slope).astype(BF16)
            tall.put(step, dot_tn(hid[...], grad_ref[...]))
            wide.put(step, dot_tn(act_ref[...], dz_ref[...]))

        @pl.when(step == 0)
        def _():
            pl.semaphore_wait(barrier, 4)

        for stage in (3, 2, 1, 0):
            chunk = step - 1 - stage

            @pl.when(jnp.logical_and(chunk >= 0, chunk < count))
            def _():
                for red in (tall, wide):
                    red.add(chunk, stage)

        for stage in (3, 2, 1, 0):
            chunk = step - stage

            @pl.when(jnp.logical_and(chunk >= 0, chunk < count))
            def _():
                for red in (tall, wide):
                    red.send(chunk, stage)

        @pl.when(step >= 4)
        def _():
            tall_ref[0] = tall.result(step - 4)
            wide_ref[...] = wide.result(step - 4)

    last = count - 1
    up_spec = (
        pl.BlockSpec((d, CHUNK), lambda i: (0, low + jnp.minimum(i, last)))
        if pre is None
        else pl.BlockSpec((rows, CHUNK), lambda i: (0, low + jnp.minimum(i, last)))
    )
    return pl.pallas_call(
        kernel,
        grid=(count + 4,),
        in_specs=[
            whole((rows, d)), whole((rows, d)), up_spec,
            pl.BlockSpec((CHUNK, d), lambda i: (low + jnp.minimum(i, last), 0)),
        ],
        out_specs=[
            pl.BlockSpec((rows, CHUNK), lambda i: (0, jnp.minimum(i, last))),
            pl.BlockSpec((1, CHUNK // 16, d), lambda i: (jnp.maximum(i - 4, 0), 0, 0)),
            pl.BlockSpec((d // 16, CHUNK), lambda i: (0, jnp.maximum(i - 4, 0))),
        ],
        out_shape=[
            shape_of((rows, count * CHUNK), BF16),
            shape_of((count, CHUNK // 16, d), F32),
            shape_of((d // 16, count * CHUNK), F32),
        ],
        scratch_shapes=[pltpu.VMEM((rows, CHUNK), BF16)] + tall.scratch() + wide.scratch(),
        cost_estimate=cost((8 if pre is None else 6) * rows * d * CHUNK * count),
        compiler_params=pltpu.CompilerParams(vmem_limit_bytes=VMEM_LIMIT, collective_id=ident, has_side_effects=True),
    )(act, grad, w_up if pre is None else pre, w_down)


def skip_grad(grads, weight, skip, split):
    rows, d = skip.shape
    f = weight.shape[1]
    tile = 512
    half = rows // tile // 2
    widths = [part.shape[1] for part in grads]
    starts = [sum(widths[:k]) for k in range(len(widths))]

    def kernel(*refs):
        step = pl.program_id(0)
        parts, w, s, outs = refs[: len(grads)], refs[len(grads)], refs[len(grads) + 1], refs[len(grads) + 2 :]
        val = s[...].astype(F32)
        for part, start, width in zip(parts, starts, widths):
            val = val + dot_nt(part[...], w[:, start : start + width])
        val = val.astype(BF16)
        if not split:
            outs[0][...] = val
            return

        @pl.when(step < half)
        def _():
            outs[0][...] = val

        @pl.when(step >= half)
        def _():
            outs[1][...] = val

    if split:
        shapes = [shape_of((rows // 2, d), BF16)] * 2
        specs = [pl.BlockSpec((tile, d), lambda i: (jnp.minimum(i, half - 1), 0)),
                 pl.BlockSpec((tile, d), lambda i: (jnp.maximum(i - half, 0), 0))]
    else:
        shapes, specs = [shape_of((rows, d), BF16)], [row_block(tile, d)]
    return pl.pallas_call(
        kernel,
        grid=(rows // tile,),
        in_specs=[row_block(tile, width) for width in widths] + [whole((d, f)), row_block(tile, d)],
        out_specs=specs,
        out_shape=shapes,
        cost_estimate=cost(2 * rows * d * f),
        compiler_params=pltpu.CompilerParams(vmem_limit_bytes=VMEM_LIMIT),
    )(*grads, weight, skip)


def solution(mesh):
    row_spec = P(AXES, None)
    rep_spec = P(None, None)

    def gather(shard):
        return lax.all_gather(shard, AXES, axis=0, tiled=True)

    def pair_grads(act, grad, w_up, pre, w_down, cuts, ident):
        d = act.shape[1]
        dz, talls, wides = [], [], []
        for k, (low, high) in enumerate(zip(cuts[:-1], cuts[1:])):
            part, tall, wide = column_grads(act, grad, w_up, pre, w_down, low, high - low, ident + k)
            act, *_ = lax.optimization_barrier((act, tall, wide))
            dz.append(part)
            gathered_tall = gather(tall)
            wides.append(gather(wide))
            tall = gathered_tall.reshape(16, high - low, CHUNK // 16, d)
            talls.append(tall.transpose(1, 0, 2, 3).reshape((high - low) * CHUNK, d))
        return dz, talls, wides

    def step(x_one, g_one, x_two, g_two, w_one, w_two, w_three, w_four):
        xc, gc, p1, h2 = forward(x_one, x_two, g_one, g_two, w_one, w_two)
        dz3, four, three = pair_grads(h2, gc, w_three, None, w_four, CUTS_UPPER, 1)
        (dh2,) = skip_grad(dz3, w_three, gc, False)
        dz1, two, one = pair_grads(xc, dh2, None, p1, w_two, CUTS_LOWER, 4)
        dx_one, dx_two = skip_grad(dz1, w_one, dh2, True)
        dw_four, dw_two = jnp.concatenate(four, axis=0), jnp.concatenate(two, axis=0)
        dw_three, dw_one = jnp.concatenate(three, axis=1), jnp.concatenate(one, axis=1)
        return dw_one, dw_two, dw_three, dw_four, dx_one, dx_two

    return jax.shard_map(
        step,
        mesh=mesh,
        in_specs=(row_spec, row_spec, row_spec, row_spec, rep_spec, rep_spec, rep_spec, rep_spec),
        out_specs=(rep_spec, rep_spec, rep_spec, rep_spec, row_spec, row_spec),
        check_vma=False,
    )
```

```python
import jax
import jax.numpy as jnp
from jax import lax
from jax.experimental import pallas as pl
from jax.experimental.pallas import tpu as pltpu
from jax.sharding import PartitionSpec as P

GELU_C = 0.7978845608028654
GELU_A = 0.044715
AXES = ("dz", "dy", "dx")
BF16 = jnp.bfloat16
F32 = jnp.float32
VMEM_LIMIT = 64000000
MESH = pl.DeviceIdType.MESH
CHUNK = 256
EARLY_UPPER = 5
EARLY_LOWER = 6
COLOUR_AXES = ((2, 1, 0), (1, 0, 2), (0, 2, 1))


def gelu_value(pre_act):
    pre_f = pre_act.astype(F32)
    return 0.5 * pre_f * (1.0 + jnp.tanh(GELU_C * (pre_f + GELU_A * pre_f * pre_f * pre_f)))


def gelu_both(val):
    square = val * val
    tanh_val = jnp.tanh(val * (GELU_C + (GELU_C * GELU_A) * square))
    half = 0.5 * val
    curve = half * (GELU_C + (3.0 * GELU_C * GELU_A) * square)
    return half + half * tanh_val, (0.5 + 0.5 * tanh_val) + curve * (1.0 - tanh_val * tanh_val)


def dot_nn(lhs, rhs):
    return lax.dot_general(lhs, rhs, (((1,), (0,)), ((), ())), preferred_element_type=F32)


def dot_nt(lhs, rhs):
    return lax.dot_general(lhs, rhs, (((1,), (1,)), ((), ())), preferred_element_type=F32)


def dot_tn(lhs, rhs):
    return lax.dot_general(lhs, rhs, (((0,), (0,)), ((), ())), preferred_element_type=F32)


class Reducer:
    def __init__(self, d, early):
        self.early = early
        self.slots = 10 if early else 5
        self.half = CHUNK // 16
        self.rows, self.cols = 2 * self.half, d
        tiles = d // 128
        sizes = [(tiles // 3 + (1 if k < tiles % 3 else 0)) * 128 for k in range(3)]
        self.parts = [(sum(sizes[:k]), sizes[k]) for k in range(3)]

    def scratch(self):
        bufs = [
            pltpu.VMEM((self.slots, 2, 2, 2, 2, self.rows, self.cols), F32),
            pltpu.VMEM((2, 2, 2, 2, self.rows, self.cols), F32),
        ]
        for _, size in self.parts:
            bufs += [pltpu.VMEM((2,) + (2,) * (2 - level) + (self.rows, size), F32) for level in range(3)]
        sems = [pltpu.SemaphoreType.DMA((2, 10)), pltpu.SemaphoreType.DMA((2, 10))]
        if self.early:
            sems += [pltpu.SemaphoreType.DMA((2, 10)), pltpu.SemaphoreType.DMA((2, 10)), pltpu.SemaphoreType.DMA((2,))]
        return bufs + sems

    def bind(self, refs, place):
        self.part, self.recv0 = refs[0], refs[1]
        self.land = [refs[2 + 3 * k : 5 + 3 * k] for k in range(3)]
        self.send_sem, self.recv_sem = refs[11], refs[12]
        if self.early:
            self.out_sem, self.in_sem, self.local_sem = refs[13:]
        self.core, self.coord, self.partner, self.neighbour = place

    def put_tall(self, chunk, value):
        shape = (2, 2, 2, 2, self.half, self.cols)
        self.part[lax.rem(chunk, self.slots), :, :, :, :, : self.half, :] = value.reshape(shape)

    def put_wide(self, chunk, value):
        pieces = value.reshape(2, 2, 2, 2, self.cols // CHUNK, self.half, CHUNK)
        for q in range(self.cols // CHUNK):
            where = (lax.rem(chunk, self.slots),) + (slice(None),) * 4 + (slice(self.half, None), slice(q * CHUNK, (q + 1) * CHUNK))
            self.part[where] = pieces[:, :, :, :, q]

    def core_copy(self, chunk):
        par = lax.rem(chunk, 2)
        return pltpu.make_async_remote_copy(
            self.part.at[lax.rem(chunk, self.slots), :, :, :, 1 - self.core], self.recv0.at[par],
            self.send_sem.at[par, 9], self.recv_sem.at[par, 9], device_id=self.partner, device_id_type=MESH,
        )

    def where(self, chunk, colour, level, other):
        order = COLOUR_AXES[colour]
        index = [slice(None)] * 3
        for pos in range(level + 1):
            axis = order[pos]
            index[axis] = 1 - self.coord[axis] if (other and pos == level) else self.coord[axis]
        start, size = self.parts[colour]
        return (lax.rem(chunk, self.slots),) + tuple(index) + (self.core, slice(None), pl.ds(start, size))

    def chip_copy(self, chunk, colour, level):
        slot, par = 3 * colour + level, lax.rem(chunk, 2)
        return pltpu.make_async_remote_copy(
            self.part.at[self.where(chunk, colour, level, True)], self.land[colour][level].at[par],
            self.send_sem.at[par, slot], self.recv_sem.at[par, slot],
            device_id=self.neighbour[COLOUR_AXES[colour][level]], device_id_type=MESH,
        )

    def send(self, chunk, stage):
        if stage == 0:
            self.core_copy(chunk).start()
        else:
            for colour in range(3):
                self.chip_copy(chunk, colour, stage - 1).start()

    def add(self, chunk, stage):
        slot, par = lax.rem(chunk, self.slots), lax.rem(chunk, 2)
        if stage == 0:
            self.core_copy(chunk).wait()
            for z in range(2):
                for y in range(2):
                    self.part[slot, z, y, :, self.core] = self.part[slot, z, y, :, self.core] + self.recv0[par, z, y]
        else:
            for colour in range(3):
                self.chip_copy(chunk, colour, stage - 1).wait()
                mine = self.where(chunk, colour, stage - 1, False)
                self.part[mine] = self.part[mine] + self.land[colour][stage - 1][par]

    def shard(self, chunk):
        return (lax.rem(chunk, self.slots),) + tuple(self.coord) + (self.core,)

    def spread_copies(self, chunk, stage):
        par = lax.rem(chunk, 2)
        if stage == 3:
            here = self.part.at[lax.rem(chunk, self.slots), :, :, :, self.core]
            return [pltpu.make_async_remote_copy(
                here, here, self.out_sem.at[par, 9], self.in_sem.at[par, 9],
                device_id=self.partner, device_id_type=MESH,
            )]
        level = 2 - stage
        copies = []
        for colour in range(3):
            here = self.part.at[self.where(chunk, colour, level, False)]
            slot = 3 * colour + level
            copies.append(pltpu.make_async_remote_copy(
                here, here, self.out_sem.at[par, slot], self.in_sem.at[par, slot],
                device_id=self.neighbour[COLOUR_AXES[colour][level]], device_id_type=MESH,
            ))
        return copies

    def store_copy(self, chunk, full_ref):
        return pltpu.make_async_copy(
            self.part.at[lax.rem(chunk, self.slots)], full_ref.at[chunk], self.local_sem.at[lax.rem(chunk, 2)]
        )


def whole(shape):
    return pl.BlockSpec(shape, lambda i: (0,) * len(shape), pipeline_mode=pl.Buffered(1))


def row_block(tile, cols):
    return pl.BlockSpec((tile, cols), lambda i: (i, 0))


def shape_of(shape, dtype):
    return jax.ShapeDtypeStruct(shape, dtype)


def cost(flops):
    return pl.CostEstimate(flops=flops, bytes_accessed=60000000, transcendentals=0)


def forward(x_one, x_two, g_one, g_two, w_one, w_two):
    half, d = x_one.shape
    f = w_one.shape[1]
    rows, tile = 2 * half, 512
    switch = half // tile

    def kernel(x1, x2, g1, g2, w1, w2, xc, gc, p1, h2, act):
        step = pl.program_id(0)

        @pl.when(step < switch)
        def _():
            xc[...] = x1[...]
            gc[...] = g1[...]

        @pl.when(step >= switch)
        def _():
            xc[...] = x2[...]
            gc[...] = g2[...]

        for j in range(f // CHUNK):
            cs = pl.ds(j * CHUNK, CHUNK)
            pre = dot_nn(xc[...], w1[:, cs]).astype(BF16)
            p1[:, cs] = pre
            act[:, cs] = gelu_value(pre).astype(BF16)
        h2[...] = (dot_nn(act[...], w2[...]) + xc[...].astype(F32)).astype(BF16)

    first = pl.BlockSpec((tile, d), lambda i: (jnp.minimum(i, switch - 1), 0))
    second = pl.BlockSpec((tile, d), lambda i: (jnp.maximum(i - switch, 0), 0))
    narrow = shape_of((rows, d), BF16)
    return pl.pallas_call(
        kernel,
        name="forward",
        grid=(rows // tile,),
        in_specs=[first, second, first, second, whole((d, f)), whole((f, d))],
        out_specs=[row_block(tile, d), row_block(tile, d), row_block(tile, f), row_block(tile, d)],
        out_shape=[narrow, narrow, shape_of((rows, f), BF16), narrow],
        scratch_shapes=[pltpu.VMEM((tile, f), BF16)],
        cost_estimate=cost(4 * rows * d * f),
        compiler_params=pltpu.CompilerParams(vmem_limit_bytes=VMEM_LIMIT),
    )(x_one, x_two, g_one, g_two, w_one, w_two)


def column_grads(act, grad, w_up, pre, w_down, ident, early, shift):
    rows, d = act.shape
    f = w_down.shape[0]
    count = f // CHUNK
    red = Reducer(d, early)
    tile = 512

    def kernel(act_ref, grad_ref, src_ref, down_ref, dz_ref, shard_ref, *refs):
        if early:
            full_ref, refs = refs[0], refs[1:]
        hid, refs = refs[0], refs[1:]
        step = pl.program_id(0)
        dx_pos = lax.axis_index("dx")
        core = lax.rem(dx_pos, 2)
        coord = [lax.axis_index("dz"), lax.axis_index("dy"), dx_pos // 2]
        partner = {"dx": dx_pos + 1 - 2 * core}
        neighbour = [{"dz": 1 - coord[0]}, {"dy": 1 - coord[1]}, {"dx": lax.rem(dx_pos + 2, 4)}]
        place = (core, coord, partner, neighbour)
        red.bind(refs, place)
        barrier = pltpu.get_barrier_semaphore()

        @pl.when(step == 0)
        def _():
            for other in [partner] + neighbour:
                pl.semaphore_signal(barrier, inc=1, device_id=other, device_id_type=MESH)

        @pl.when(step < count)
        def _():
            for r in range(rows // tile):
                rs = pl.ds(r * tile, tile)
                if pre is None:
                    val = dot_nn(act_ref[rs, :], src_ref[...]).astype(BF16).astype(F32)
                else:
                    val = src_ref[rs, :].astype(F32)
                hid_val, slope = gelu_both(val)
                hid[rs, :] = hid_val.astype(BF16)
                dz_ref[rs, :] = (dot_nt(grad_ref[rs, :], down_ref[...]) * slope).astype(BF16)
            red.put_tall(step, dot_tn(hid[...], grad_ref[...]))
            red.put_wide(step, dot_tn(act_ref[...], dz_ref[...]))

        @pl.when(step == 0)
        def _():
            pl.semaphore_wait(barrier, 4)

        def at(chunk, limit):
            return pl.when(jnp.logical_and(chunk >= 0, chunk < limit))

        if early:
            for stage in (3, 2, 1, 0):
                @at(step - 6 - stage, early)
                def _():
                    for copy in red.spread_copies(step - 6 - stage, stage):
                        copy.wait()

        for stage in (3, 2, 1, 0):
            @at(step - 1 - stage, count)
            def _():
                red.add(step - 1 - stage, stage)

        @pl.when(step >= 4)
        def _():
            mine = red.shard(step - 4)
            final = red.part[mine] * (1.0 / 16.0)
            red.part[mine] = final
            shard_ref[0] = final

        if early:
            @at(step - 9, early)
            def _():
                red.store_copy(step - 9, full_ref).start()

        for stage in (3, 2, 1, 0):
            @at(step - stage, count)
            def _():
                red.send(step - stage, stage)

        if early:
            for stage in (3, 2, 1, 0):
                @at(step - 5 - stage, early)
                def _():
                    for copy in red.spread_copies(step - 5 - stage, stage):
                        copy.start()

            @at(step - 9, early)
            def _():
                red.store_copy(step - 9, full_ref).wait()

    last = count - 1

    def at_chunk(i):
        return lax.rem(jnp.minimum(i, last) + shift, count)

    up_spec = pl.BlockSpec((d if pre is None else rows, CHUNK), lambda i: (0, at_chunk(i)))
    return pl.pallas_call(
        kernel,
        grid=(count + 4,),
        in_specs=[
            whole((rows, d)), whole((rows, d)), up_spec,
            pl.BlockSpec((CHUNK, d), lambda i: (at_chunk(i), 0)),
        ],
        out_specs=[
            pl.BlockSpec((rows, CHUNK), lambda i: (0, at_chunk(i))),
            pl.BlockSpec((1, CHUNK // 8, d), lambda i: (jnp.maximum(i - 4 - early, 0), 0, 0)),
        ] + ([pl.BlockSpec(memory_space=pl.ANY)] if early else []),
        out_shape=[
            shape_of((rows, count * CHUNK), BF16),
            shape_of((count - early, CHUNK // 8, d), F32),
        ] + ([shape_of((early, 2, 2, 2, 2, CHUNK // 8, d), F32)] if early else []),
        scratch_shapes=[pltpu.VMEM((rows, CHUNK), BF16)] + red.scratch(),
        cost_estimate=cost((8 if pre is None else 6) * rows * d * CHUNK * count),
        compiler_params=pltpu.CompilerParams(vmem_limit_bytes=VMEM_LIMIT, collective_id=ident, has_side_effects=True),
    )(act, grad, w_up if pre is None else pre, w_down)


def skip_grad(grad, weight, skip, split, places=()):
    rows, d = skip.shape
    f = weight.shape[1]
    tile = 512
    half = rows // tile // 2
    steps = rows // tile
    if split:
        shapes = [shape_of((rows // 2, d), BF16)] * 2
        specs = [pl.BlockSpec((tile, d), lambda i: (jnp.minimum(i, half - 1), 0)),
                 pl.BlockSpec((tile, d), lambda i: (jnp.maximum(i - half, 0), 0))]
    else:
        shapes, specs = [shape_of((rows, d), BF16)], [row_block(tile, d)]
    arrays, in_specs, slots = [], [], []
    group = 16 // steps
    for parts, runs in places:
        more, more_specs, place_out, place_shapes = place_specs(parts, runs, f // CHUNK, d, group)
        slots.append((3 + len(arrays), len(more), len(shapes), runs))
        arrays, in_specs = arrays + more, in_specs + more_specs
        shapes, specs = shapes + place_shapes, specs + place_out
    n_in = 3 + len(arrays)

    def kernel(*refs):
        step = pl.program_id(0)
        z, w, s = refs[:3]
        outs = refs[n_in:]
        val = dot_nt(z[...], w[...]) + s[...].astype(F32)
        val = val.astype(BF16)
        for first, n_parts, out, runs in slots:
            for device in range(group):
                place_shards(refs[first : first + n_parts], runs, outs[out], outs[out + 1], device)
        if not split:
            outs[0][...] = val
            return

        @pl.when(step < half)
        def _():
            outs[0][...] = val

        @pl.when(step >= half)
        def _():
            outs[1][...] = val

    return pl.pallas_call(
        kernel,
        grid=(steps,),
        in_specs=[row_block(tile, f), whole((d, f)), row_block(tile, d)] + in_specs,
        out_specs=specs,
        out_shape=shapes,
        cost_estimate=cost(2 * rows * d * f),
        compiler_params=pltpu.CompilerParams(vmem_limit_bytes=VMEM_LIMIT),
    )(grad, weight, skip, *arrays)


def place_shards(refs, runs, tall, wide, device):
    half = CHUNK // 16
    pieces = tall.shape[3] // CHUNK
    base = device * pieces * half
    for ref, (low, high, by_chunk) in zip(refs, runs):
        for j in range(high - low):
            block = ref[j, device] if by_chunk else ref[device, j]
            tall[low + j, device] = block[:half]
            for q in range(pieces):
                cols = slice((low + j) * CHUNK, (low + j + 1) * CHUNK)
                wide[base + q * half : base + (q + 1) * half, cols] = block[half:, q * CHUNK : (q + 1) * CHUNK]


def place_specs(parts, runs, total, d, group, shown=None):
    half = CHUNK // 16
    arrays, in_specs = [], []
    for part, (low, high, by_chunk) in zip(parts, runs):
        if by_chunk:
            arrays.append(part.reshape(high - low, 16, 2 * half, d))
            in_specs.append(pl.BlockSpec((high - low, group, 2 * half, d), lambda i: (0, i, 0, 0)))
        else:
            arrays.append(part.reshape(16, high - low, 2 * half, d))
            in_specs.append(pl.BlockSpec((group, high - low, 2 * half, d), lambda i: (i, 0, 0, 0)))
    shown = shown or total
    out_specs = [
        pl.BlockSpec((shown, group, half, d), lambda i: (0, i, 0, 0)),
        pl.BlockSpec((group * d // 16, shown * CHUNK), lambda i: (i, 0)),
    ]
    shapes = [shape_of((total, 16, half, d), F32), shape_of((d, total * CHUNK), F32)]
    return arrays, in_specs, out_specs, shapes


def assemble(parts, runs, total, d, into):
    arrays, in_specs, out_specs, shapes = place_specs(parts, runs, total, d, 1, runs[-1][1])
    n_parts = len(arrays)

    def kernel(*refs):
        place_shards(refs[:n_parts], runs, refs[-2], refs[-1], 0)

    return pl.pallas_call(
        kernel,
        grid=(16,),
        in_specs=in_specs + [pl.BlockSpec(memory_space=pl.ANY)] * 2,
        out_specs=out_specs,
        out_shape=shapes,
        input_output_aliases={n_parts: 0, n_parts + 1: 1},
        cost_estimate=pl.CostEstimate(flops=2000000000, bytes_accessed=16 * total * CHUNK * d, transcendentals=0),
        compiler_params=pltpu.CompilerParams(vmem_limit_bytes=VMEM_LIMIT),
    )(*arrays, *into)


def solution(mesh):
    row_spec = P(AXES, None)
    rep_spec = P(None, None)

    def gather(shard):
        return lax.all_gather(shard, AXES, axis=0, tiled=True)

    def step(x_one, g_one, x_two, g_two, w_one, w_two, w_three, w_four):
        xc, gc, p1, h2 = forward(x_one, x_two, g_one, g_two, w_one, w_two)
        f, d = w_four.shape
        total = f // CHUNK
        dz3, shard, up_first = column_grads(h2, gc, w_three, None, w_four, 1, EARLY_UPPER, 0)
        up_rest = gather(shard)
        (dh2,) = skip_grad(dz3, w_three, gc, False)
        shift = total - EARLY_LOWER
        dz1, shard, low_first = column_grads(xc, dh2, None, p1, w_two, 2, EARLY_LOWER, shift)
        low_rest = gather(shard)
        dx_one, dx_two, four, dw_three, two, dw_one = skip_grad(
            dz1, w_one, dh2, True,
            (((up_first, up_rest), ((0, EARLY_UPPER, True), (EARLY_UPPER, total, False))), ((low_first,), ((shift, total, True),))),
        )
        two, dw_one = assemble((low_rest,), ((0, shift, False),), total, d, (two, dw_one))
        dw_four, dw_two = four.reshape(f, d), two.reshape(f, d)
        return dw_one, dw_two, dw_three, dw_four, dx_one, dx_two

    return jax.shard_map(
        step,
        mesh=mesh,
        in_specs=(row_spec, row_spec, row_spec, row_spec, rep_spec, rep_spec, rep_spec, rep_spec),
        out_specs=(rep_spec, rep_spec, rep_spec, rep_spec, row_spec, row_spec),
        check_vma=False,
    )
```

```python
import jax
import jax.numpy as jnp
from jax import lax
from jax.experimental import pallas as pl
from jax.experimental.pallas import tpu as pltpu
from jax.sharding import PartitionSpec as P

GELU_C = 0.7978845608028654
GELU_A = 0.044715
AXES = ("dz", "dy", "dx")
BF16 = jnp.bfloat16
F32 = jnp.float32
VMEM_LIMIT = 64000000
MESH = pl.DeviceIdType.MESH
CHUNK = 256
EARLY_UPPER = 3
EARLY_LOWER = 5
COLOUR_AXES = ((2, 1, 0), (1, 0, 2), (0, 2, 1))


def gelu_value(pre_act):
    pre_f = pre_act.astype(F32)
    return 0.5 * pre_f * (1.0 + jnp.tanh(GELU_C * (pre_f + GELU_A * pre_f * pre_f * pre_f)))


def gelu_both(val):
    square = val * val
    tanh_val = jnp.tanh(val * (GELU_C + (GELU_C * GELU_A) * square))
    half = 0.5 * val
    curve = half * (GELU_C + (3.0 * GELU_C * GELU_A) * square)
    return half + half * tanh_val, (0.5 + 0.5 * tanh_val) + curve * (1.0 - tanh_val * tanh_val)


def dot_nn(lhs, rhs):
    return lax.dot_general(lhs, rhs, (((1,), (0,)), ((), ())), preferred_element_type=F32)


def dot_nt(lhs, rhs):
    return lax.dot_general(lhs, rhs, (((1,), (1,)), ((), ())), preferred_element_type=F32)


def dot_tn(lhs, rhs):
    return lax.dot_general(lhs, rhs, (((0,), (0,)), ((), ())), preferred_element_type=F32)


class Reducer:
    def __init__(self, d, early):
        self.early = early
        self.slots = 10 if early else 5
        self.half = CHUNK // 16
        self.rows, self.cols = 2 * self.half, d
        tiles = d // 128
        sizes = [(tiles // 3 + (1 if k < tiles % 3 else 0)) * 128 for k in range(3)]
        self.parts = [(sum(sizes[:k]), sizes[k]) for k in range(3)]

    def scratch(self):
        bufs = [
            pltpu.VMEM((self.slots, 2, 2, 2, 2, self.rows, self.cols), F32),
            pltpu.VMEM((2, 2, 2, 2, self.rows, self.cols), F32),
        ]
        for _, size in self.parts:
            bufs += [pltpu.VMEM((2,) + (2,) * (2 - level) + (self.rows, size), F32) for level in range(3)]
        sems = [pltpu.SemaphoreType.DMA((2, 10)), pltpu.SemaphoreType.DMA((2, 10))]
        if self.early:
            sems += [pltpu.SemaphoreType.DMA((2, 10)), pltpu.SemaphoreType.DMA((2, 10)), pltpu.SemaphoreType.DMA((2,))]
        return bufs + sems

    def bind(self, refs, place):
        self.part, self.recv0 = refs[0], refs[1]
        self.land = [refs[2 + 3 * k : 5 + 3 * k] for k in range(3)]
        self.send_sem, self.recv_sem = refs[11], refs[12]
        if self.early:
            self.out_sem, self.in_sem, self.local_sem = refs[13:]
        self.core, self.coord, self.partner, self.neighbour = place

    def put_tall(self, chunk, value):
        shape = (2, 2, 2, 2, self.half, self.cols)
        self.part[lax.rem(chunk, self.slots), :, :, :, :, : self.half, :] = value.reshape(shape)

    def put_wide(self, chunk, value):
        pieces = value.reshape(2, 2, 2, 2, self.cols // CHUNK, self.half, CHUNK)
        for q in range(self.cols // CHUNK):
            where = (lax.rem(chunk, self.slots),) + (slice(None),) * 4 + (slice(self.half, None), slice(q * CHUNK, (q + 1) * CHUNK))
            self.part[where] = pieces[:, :, :, :, q]

    def core_copy(self, chunk):
        par = lax.rem(chunk, 2)
        return pltpu.make_async_remote_copy(
            self.part.at[lax.rem(chunk, self.slots), :, :, :, 1 - self.core], self.recv0.at[par],
            self.send_sem.at[par, 9], self.recv_sem.at[par, 9], device_id=self.partner, device_id_type=MESH,
        )

    def where(self, chunk, colour, level, other):
        order = COLOUR_AXES[colour]
        index = [slice(None)] * 3
        for pos in range(level + 1):
            axis = order[pos]
            index[axis] = 1 - self.coord[axis] if (other and pos == level) else self.coord[axis]
        start, size = self.parts[colour]
        return (lax.rem(chunk, self.slots),) + tuple(index) + (self.core, slice(None), pl.ds(start, size))

    def chip_copy(self, chunk, colour, level):
        slot, par = 3 * colour + level, lax.rem(chunk, 2)
        return pltpu.make_async_remote_copy(
            self.part.at[self.where(chunk, colour, level, True)], self.land[colour][level].at[par],
            self.send_sem.at[par, slot], self.recv_sem.at[par, slot],
            device_id=self.neighbour[COLOUR_AXES[colour][level]], device_id_type=MESH,
        )

    def send(self, chunk, stage):
        if stage == 0:
            self.core_copy(chunk).start()
        else:
            for colour in range(3):
                self.chip_copy(chunk, colour, stage - 1).start()

    def add(self, chunk, stage):
        slot, par = lax.rem(chunk, self.slots), lax.rem(chunk, 2)
        if stage == 0:
            self.core_copy(chunk).wait()
            for z in range(2):
                for y in range(2):
                    self.part[slot, z, y, :, self.core] = self.part[slot, z, y, :, self.core] + self.recv0[par, z, y]
        else:
            for colour in range(3):
                self.chip_copy(chunk, colour, stage - 1).wait()
                mine = self.where(chunk, colour, stage - 1, False)
                self.part[mine] = self.part[mine] + self.land[colour][stage - 1][par]

    def shard(self, chunk):
        return (lax.rem(chunk, self.slots),) + tuple(self.coord) + (self.core,)

    def spread_copies(self, chunk, stage):
        par = lax.rem(chunk, 2)
        if stage == 3:
            here = self.part.at[lax.rem(chunk, self.slots), :, :, :, self.core]
            return [pltpu.make_async_remote_copy(
                here, here, self.out_sem.at[par, 9], self.in_sem.at[par, 9],
                device_id=self.partner, device_id_type=MESH,
            )]
        level = 2 - stage
        copies = []
        for colour in range(3):
            here = self.part.at[self.where(chunk, colour, level, False)]
            slot = 3 * colour + level
            copies.append(pltpu.make_async_remote_copy(
                here, here, self.out_sem.at[par, slot], self.in_sem.at[par, slot],
                device_id=self.neighbour[COLOUR_AXES[colour][level]], device_id_type=MESH,
            ))
        return copies

    def store_copy(self, chunk, full_ref):
        return pltpu.make_async_copy(
            self.part.at[lax.rem(chunk, self.slots)], full_ref.at[chunk], self.local_sem.at[lax.rem(chunk, 2)]
        )


def whole(shape):
    return pl.BlockSpec(shape, lambda i: (0,) * len(shape), pipeline_mode=pl.Buffered(1))


def row_block(tile, cols):
    return pl.BlockSpec((tile, cols), lambda i: (i, 0))


def shape_of(shape, dtype):
    return jax.ShapeDtypeStruct(shape, dtype)


def cost(flops):
    return pl.CostEstimate(flops=flops, bytes_accessed=60000000, transcendentals=0)


def forward(x_one, x_two, g_one, g_two, w_one, w_two):
    half, d = x_one.shape
    f = w_one.shape[1]
    rows, tile = 2 * half, 512
    switch = half // tile

    def kernel(x1, x2, g1, g2, w1, w2, xc, gc, p1, h2, act):
        step = pl.program_id(0)

        @pl.when(step < switch)
        def _():
            xc[...] = x1[...]
            gc[...] = g1[...]

        @pl.when(step >= switch)
        def _():
            xc[...] = x2[...]
            gc[...] = g2[...]

        for j in range(f // CHUNK):
            cs = pl.ds(j * CHUNK, CHUNK)
            pre = dot_nn(xc[...], w1[:, cs]).astype(BF16)
            p1[:, cs] = pre
            act[:, cs] = gelu_value(pre).astype(BF16)
        h2[...] = (dot_nn(act[...], w2[...]) + xc[...].astype(F32)).astype(BF16)

    first = pl.BlockSpec((tile, d), lambda i: (jnp.minimum(i, switch - 1), 0))
    second = pl.BlockSpec((tile, d), lambda i: (jnp.maximum(i - switch, 0), 0))
    narrow = shape_of((rows, d), BF16)
    return pl.pallas_call(
        kernel,
        name="forward",
        grid=(rows // tile,),
        in_specs=[first, second, first, second, whole((d, f)), whole((f, d))],
        out_specs=[row_block(tile, d), row_block(tile, d), row_block(tile, f), row_block(tile, d)],
        out_shape=[narrow, narrow, shape_of((rows, f), BF16), narrow],
        scratch_shapes=[pltpu.VMEM((tile, f), BF16)],
        cost_estimate=cost(4 * rows * d * f),
        compiler_params=pltpu.CompilerParams(vmem_limit_bytes=VMEM_LIMIT),
    )(x_one, x_two, g_one, g_two, w_one, w_two)


def column_grads(act, grad, w_up, pre, w_down, ident, early, shift):
    rows, d = act.shape
    f = w_down.shape[0]
    count = f // CHUNK
    red = Reducer(d, early)
    tile = 512

    def kernel(act_ref, grad_ref, src_ref, down_ref, dz_ref, shard_ref, *refs):
        if early:
            full_ref, refs = refs[0], refs[1:]
        hid, refs = refs[0], refs[1:]
        step = pl.program_id(0)
        dx_pos = lax.axis_index("dx")
        core = lax.rem(dx_pos, 2)
        coord = [lax.axis_index("dz"), lax.axis_index("dy"), dx_pos // 2]
        partner = {"dx": dx_pos + 1 - 2 * core}
        neighbour = [{"dz": 1 - coord[0]}, {"dy": 1 - coord[1]}, {"dx": lax.rem(dx_pos + 2, 4)}]
        place = (core, coord, partner, neighbour)
        red.bind(refs, place)
        barrier = pltpu.get_barrier_semaphore()

        @pl.when(step == 0)
        def _():
            for other in [partner] + neighbour:
                pl.semaphore_signal(barrier, inc=1, device_id=other, device_id_type=MESH)

        @pl.when(step < count)
        def _():
            if pre is None:
                for r in range(rows // tile):
                    rs = pl.ds(r * tile, tile)
                    hid[rs, :] = dot_nn(act_ref[rs, :], src_ref[...]).astype(BF16)
            for r in range(rows // tile):
                rs = pl.ds(r * tile, tile)
                val = (hid if pre is None else src_ref)[rs, :].astype(F32)
                hid_val, slope = gelu_both(val)
                hid[rs, :] = hid_val.astype(BF16)
                dz_ref[rs, :] = (dot_nt(grad_ref[rs, :], down_ref[...]) * slope).astype(BF16)
            red.put_tall(step, dot_tn(hid[...], grad_ref[...]))
            red.put_wide(step, dot_tn(act_ref[...], dz_ref[...]))

        @pl.when(step == 0)
        def _():
            pl.semaphore_wait(barrier, 4)

        def at(chunk, limit):
            return pl.when(jnp.logical_and(chunk >= 0, chunk < limit))

        if early:
            for stage in (3, 2, 1, 0):
                @at(step - 6 - stage, early)
                def _():
                    for copy in red.spread_copies(step - 6 - stage, stage):
                        copy.wait()

        for stage in (3, 2, 1, 0):
            @at(step - 1 - stage, count)
            def _():
                red.add(step - 1 - stage, stage)

        @pl.when(step >= 4)
        def _():
            mine = red.shard(step - 4)
            final = red.part[mine] * (1.0 / 16.0)
            red.part[mine] = final
            shard_ref[0] = final

        if early:
            @at(step - 9, early)
            def _():
                red.store_copy(step - 9, full_ref).start()

        for stage in (3, 2, 1, 0):
            @at(step - stage, count)
            def _():
                red.send(step - stage, stage)

        if early:
            for stage in (3, 2, 1, 0):
                @at(step - 5 - stage, early)
                def _():
                    for copy in red.spread_copies(step - 5 - stage, stage):
                        copy.start()

            @at(step - 9, early)
            def _():
                red.store_copy(step - 9, full_ref).wait()

    last = count - 1

    def at_chunk(i):
        return lax.rem(jnp.minimum(i, last) + shift, count)

    up_spec = pl.BlockSpec((d if pre is None else rows, CHUNK), lambda i: (0, at_chunk(i)))
    return pl.pallas_call(
        kernel,
        grid=(count + 4,),
        in_specs=[
            whole((rows, d)), whole((rows, d)), up_spec,
            pl.BlockSpec((CHUNK, d), lambda i: (at_chunk(i), 0)),
        ],
        out_specs=[
            pl.BlockSpec((rows, CHUNK), lambda i: (0, at_chunk(i))),
            pl.BlockSpec((1, CHUNK // 8, d), lambda i: (jnp.maximum(i - 4 - early, 0), 0, 0)),
        ] + ([pl.BlockSpec(memory_space=pl.ANY)] if early else []),
        out_shape=[
            shape_of((rows, count * CHUNK), BF16),
            shape_of((count - early, CHUNK // 8, d), F32),
        ] + ([shape_of((early, 2, 2, 2, 2, CHUNK // 8, d), F32)] if early else []),
        scratch_shapes=[pltpu.VMEM((rows, CHUNK), BF16)] + red.scratch(),
        cost_estimate=cost((8 if pre is None else 6) * rows * d * CHUNK * count),
        compiler_params=pltpu.CompilerParams(vmem_limit_bytes=VMEM_LIMIT, collective_id=ident, has_side_effects=True),
    )(act, grad, w_up if pre is None else pre, w_down)


def skip_grad(grad, weight, skip, split, places=()):
    rows, d = skip.shape
    f = weight.shape[1]
    tile = 512
    half = rows // tile // 2
    steps = rows // tile
    if split:
        shapes = [shape_of((rows // 2, d), BF16)] * 2
        specs = [pl.BlockSpec((tile, d), lambda i: (jnp.minimum(i, half - 1), 0)),
                 pl.BlockSpec((tile, d), lambda i: (jnp.maximum(i - half, 0), 0))]
    else:
        shapes, specs = [shape_of((rows, d), BF16)], [row_block(tile, d)]
    arrays, in_specs, slots = [], [], []
    group = 16 // steps
    for parts, runs in places:
        more, more_specs, place_out, place_shapes = place_specs(parts, runs, f // CHUNK, d, group)
        slots.append((3 + len(arrays), len(more), len(shapes), runs))
        arrays, in_specs = arrays + more, in_specs + more_specs
        shapes, specs = shapes + place_shapes, specs + place_out
    n_in = 3 + len(arrays)

    def kernel(*refs):
        step = pl.program_id(0)
        z, w, s = refs[:3]
        outs = refs[n_in:]
        val = dot_nt(z[...], w[...]) + s[...].astype(F32)
        val = val.astype(BF16)
        for first, n_parts, out, runs in slots:
            for device in range(group):
                place_shards(refs[first : first + n_parts], runs, outs[out], outs[out + 1], device)
        if not split:
            outs[0][...] = val
            return

        @pl.when(step < half)
        def _():
            outs[0][...] = val

        @pl.when(step >= half)
        def _():
            outs[1][...] = val

    return pl.pallas_call(
        kernel,
        grid=(steps,),
        in_specs=[row_block(tile, f), whole((d, f)), row_block(tile, d)] + in_specs,
        out_specs=specs,
        out_shape=shapes,
        cost_estimate=cost(2 * rows * d * f),
        compiler_params=pltpu.CompilerParams(vmem_limit_bytes=VMEM_LIMIT),
    )(grad, weight, skip, *arrays)


def place_shards(refs, runs, tall, wide, device):
    half = CHUNK // 16
    pieces = tall.shape[3] // CHUNK
    base = device * pieces * half
    for ref, (low, high, by_chunk) in zip(refs, runs):
        for j in range(high - low):
            block = ref[j, device] if by_chunk else ref[device, j]
            tall[low + j, device] = block[:half]
            for q in range(pieces):
                cols = slice((low + j) * CHUNK, (low + j + 1) * CHUNK)
                wide[base + q * half : base + (q + 1) * half, cols] = block[half:, q * CHUNK : (q + 1) * CHUNK]


def place_specs(parts, runs, total, d, group, shown=None):
    half = CHUNK // 16
    arrays, in_specs = [], []
    for part, (low, high, by_chunk) in zip(parts, runs):
        if by_chunk:
            arrays.append(part.reshape(high - low, 16, 2 * half, d))
            in_specs.append(pl.BlockSpec((high - low, group, 2 * half, d), lambda i: (0, i, 0, 0)))
        else:
            arrays.append(part.reshape(16, high - low, 2 * half, d))
            in_specs.append(pl.BlockSpec((group, high - low, 2 * half, d), lambda i: (i, 0, 0, 0)))
    shown = shown or total
    out_specs = [
        pl.BlockSpec((shown, group, half, d), lambda i: (0, i, 0, 0)),
        pl.BlockSpec((group * d // 16, shown * CHUNK), lambda i: (i, 0)),
    ]
    shapes = [shape_of((total, 16, half, d), F32), shape_of((d, total * CHUNK), F32)]
    return arrays, in_specs, out_specs, shapes


def assemble(parts, runs, total, d, into):
    arrays, in_specs, out_specs, shapes = place_specs(parts, runs, total, d, 1, runs[-1][1])
    n_parts = len(arrays)

    def kernel(*refs):
        place_shards(refs[:n_parts], runs, refs[-2], refs[-1], 0)

    return pl.pallas_call(
        kernel,
        grid=(16,),
        in_specs=in_specs + [pl.BlockSpec(memory_space=pl.ANY)] * 2,
        out_specs=out_specs,
        out_shape=shapes,
        input_output_aliases={n_parts: 0, n_parts + 1: 1},
        cost_estimate=pl.CostEstimate(flops=2000000000, bytes_accessed=16 * total * CHUNK * d, transcendentals=0),
        compiler_params=pltpu.CompilerParams(vmem_limit_bytes=VMEM_LIMIT),
    )(*arrays, *into)


def solution(mesh):
    row_spec = P(AXES, None)
    rep_spec = P(None, None)

    def gather(shard):
        return lax.all_gather(shard, AXES, axis=0, tiled=True)

    def step(x_one, g_one, x_two, g_two, w_one, w_two, w_three, w_four):
        xc, gc, p1, h2 = forward(x_one, x_two, g_one, g_two, w_one, w_two)
        f, d = w_four.shape
        total = f // CHUNK
        dz3, shard, up_first = column_grads(h2, gc, w_three, None, w_four, 1, EARLY_UPPER, 0)
        up_rest = gather(shard)
        (dh2,) = skip_grad(dz3, w_three, gc, False)
        shift = total - EARLY_LOWER
        dz1, shard, low_first = column_grads(xc, dh2, None, p1, w_two, 2, EARLY_LOWER, shift)
        low_rest = gather(shard)
        dx_one, dx_two, four, dw_three, two, dw_one = skip_grad(
            dz1, w_one, dh2, True,
            (((up_first, up_rest), ((0, EARLY_UPPER, True), (EARLY_UPPER, total, False))), ((low_first,), ((shift, total, True),))),
        )
        two, dw_one = assemble((low_rest,), ((0, shift, False),), total, d, (two, dw_one))
        dw_four, dw_two = four.reshape(f, d), two.reshape(f, d)
        return dw_one, dw_two, dw_three, dw_four, dx_one, dx_two

    return jax.shard_map(
        step,
        mesh=mesh,
        in_specs=(row_spec, row_spec, row_spec, row_spec, rep_spec, rep_spec, rep_spec, rep_spec),
        out_specs=(rep_spec, rep_spec, rep_spec, rep_spec, row_spec, row_spec),
        check_vma=False,
    )
```
